256 devices in a mesh: row: 32 (over x, z_hi, core), col: 8 (over z_lo, y).
Axes of the slice: x: 4, y: 4, z: 8 (z_hi: 4, z_lo: 2; z = z_hi * 2 + z_lo), core: 2. Of those that a mesh axis runs over, the one named last changes fastest.
Arguments:
- counts: float32 [16384, 16384], P('row', 'col'), may hold values from 0 to 12, as said below
- loadings: float32 [16384, 64], P(('col', 'row')), may hold values from 0.02 to 0.4
Outputs:
- row_grad: float32 [16384, 64], P(('row', 'col'))
- col_grad: float32 [16384, 64], P(('col', 'row'))
The draws below stay inside these ranges and needn't reach their ends.
Inputs may be any that keep to these rules, and one draw needn't show every extreme that they name: `counts`: whole numbers, more of them near the diagonal.
All inputs are finite; a program needn't handle non-finite values.
Results may differ from the reference program's by a relative error of at most 0.0003.
Values sent between devices are 32-bit elements; how exact they have to be, the bound alone decides.
No kernel may reach another device: no remote copies, remote signals or barrier semaphores. Data moves between devices by JAX's collectives and lax.ppermute only.
A program may use at most 64 MiB of HBM per device.

```python
import math
import jax
import jax.numpy as jnp
from jax import lax

RANK = 64
ROWS_DEV = 512
NBINS = 16384


def draw_counts(key, part):
    first = jnp.arange(NBINS).astype(jnp.int32)
    distance = jnp.abs(first[:, None] - first[None, :])
    ceiling = 4 + 9 // (1 + distance // 64)
    values = jax.random.randint(jax.random.fold_in(key, 11), (NBINS, NBINS), 0, 1 << 20)
    return (values % ceiling).astype(jnp.float32)


def block_scale(stream_key, extent, cuts, smallest, top_value):
    def one(position, shards_of):
        steps = jax.random.uniform(jax.random.fold_in(jax.random.fold_in(stream_key, 6), position), (shards_of,), jnp.float32, smallest / len(cuts), top_value / len(cuts))
        return jnp.repeat(jnp.exp(steps), extent[position] // shards_of).reshape((-1,) + (1,) * (len(extent) - position - 1))

    factor_of = one(*cuts[0])
    for cut in cuts[1:]:
        factor_of = factor_of * one(*cut)
    return factor_of


def setup_inputs(seed: int = 0) -> dict:
    streams_of = jax.random.split(jax.random.key(seed), 3)
    counts = draw_counts(jax.random.fold_in(streams_of[2], 71), 0)
    loadings = jnp.clip(jnp.exp(math.log(0.4) - 2.9957323 * jax.random.uniform(streams_of[1], (NBINS, RANK), jnp.float32) ** block_scale(streams_of[1], (NBINS, RANK), ((0, 256),), -0.2, 0.2)), 0.02, 0.4)
    return dict(counts=counts, loadings=loadings)


def reference(counts, loadings):
    scale = 1.0 / (NBINS ** 0.5)
    columns = jnp.arange(NBINS).astype(jnp.int32)

    def one_block(carry, index):
        start = (index * ROWS_DEV).astype(jnp.int32)
        tile = lax.dynamic_slice_in_dim(counts, start, ROWS_DEV, 0)
        rowblock = lax.dynamic_slice_in_dim(loadings, start, ROWS_DEV, 0)
        rate = jnp.dot(rowblock, loadings.T, precision=lax.Precision.HIGHEST)
        positions = start + jnp.arange(ROWS_DEV).astype(jnp.int32)
        keep = jnp.abs(positions[:, None] - columns[None, :]) >= 2
        ratio = jnp.where(keep, 1.0 - tile / rate, jnp.float32(0.0))
        rowpart = jnp.dot(ratio, loadings, precision=lax.Precision.HIGHEST) * scale
        colpart = jnp.dot(ratio.T, rowblock, precision=lax.Precision.HIGHEST) * scale
        return carry + colpart, rowpart

    start_sum = jnp.zeros((NBINS, RANK), jnp.float32)
    col_grad, pieces = lax.scan(one_block, start_sum, jnp.arange(NBINS // ROWS_DEV).astype(jnp.int32))
    row_grad = pieces.reshape(NBINS, RANK)
    return row_grad, col_grad
```

```python
import jax
import jax.numpy as jnp
from jax import lax
from jax.experimental import pallas as pl
from jax.experimental.pallas import tpu as pltpu
from jax.sharding import PartitionSpec as P


CORES = 2
LINKS = 2
RING = 4
TILE = 256


def packed(chunk):
    half = chunk.shape[0] // 2
    return jnp.concatenate([chunk[:half], chunk[half:]], axis=1)


def low_lanes(shape):
    return lax.broadcasted_iota(jnp.int32, shape, 1) < shape[1] // 2


def swapped(x):
    return pltpu.roll(x, x.shape[1] // 2, 1)


def halves(x):
    low = low_lanes(x.shape)
    turned = swapped(x)
    return jnp.where(low, x, turned), jnp.where(low, turned, x)


def high_low(x):
    high = x.astype(jnp.bfloat16)
    return high, (x - high.astype(jnp.float32)).astype(jnp.bfloat16)


def place_of(row_index):
    return row_index // (RING * CORES), row_index // CORES % RING, row_index % CORES


def gradients(
    counts_hbm, here_ref, ring1_ref, ring2_ref, ring3_ref, own_ref, other_ref,
    row_own, row_other, own_out, other_out,
    counts_ref, arrived, a_ref, at_ref, b_ref, sums_ref,
):
    rows, cols = counts_ref.shape
    copies = [
        pltpu.make_async_copy(
            counts_hbm.at[:, pl.ds(n * TILE, TILE)],
            counts_ref.at[:, pl.ds(n * TILE, TILE)],
            arrived.at[n],
        )
        for n in range(cols // TILE)
    ]
    for copy in copies:
        copy.start()
    half, lanes = own_ref.shape[1:]
    chunk = 2 * half
    row_index = lax.axis_index("row")
    col_index = lax.axis_index("col")
    link, place = col_index // RING, col_index % RING
    first_core = row_index % CORES == 0
    scale = 1.0 / (rows * lax.axis_size("row")) ** 0.5
    f32 = jnp.float32

    x, z, core = place_of(row_index)
    home = x % 2 * 2 + z // 2
    for distance, ref in enumerate((here_ref, ring1_ref, ring2_ref, ring3_ref)):
        source_z = (z + 2 + home - place + distance) & (RING - 1)
        for k in range(CORES):
            j = source_z * CORES + (link ^ k)
            for part, twice in enumerate(halves(ref[k])):
                high, low = high_low(twice)
                at = pl.ds(pl.multiple_of(j * chunk + part * half, half), half)
                a_ref[at, :lanes] = high
                a_ref[at, lanes:] = low
    both = jnp.where(
        low_lanes((rows, lanes)), a_ref[:, :lanes].astype(f32), a_ref[:, lanes:].astype(f32)
    )
    at_ref[...] = both.T.astype(jnp.bfloat16)

    for p in range(cols // chunk // CORES):
        source = ((x - p // RING) & (RING - 1)) * RING + ((z - p % RING) & (RING - 1))
        for k, ref in enumerate((own_ref, other_ref)):
            j = source * CORES + (core ^ k)
            for part, twice in enumerate(halves(ref[p])):
                high = twice.astype(jnp.bfloat16).astype(f32)
                both = jnp.where(low_lanes(twice.shape), high, twice - high).astype(jnp.bfloat16)
                at = pl.ds(pl.multiple_of(j * chunk + part * half, half), half)
                b_ref[at, :lanes] = both
                b_ref[at, lanes:] = both

    apart = (
        lax.broadcasted_iota(jnp.int32, (TILE, TILE), 1)
        - lax.broadcasted_iota(jnp.int32, (TILE, TILE), 0)
        + (col_index * cols - row_index * rows)
    )
    for n in range(cols // TILE):
        at_n = pl.ds(n * TILE, TILE)
        copies[n].wait()
        col_sum = jnp.zeros((lanes, TILE), f32)
        for m in range(rows // TILE):
            at_m = pl.ds(m * TILE, TILE)
            rate = lax.dot_general(
                a_ref[at_m, :], b_ref[at_n, :], (((1,), (1,)), ((), ())), preferred_element_type=f32
            )
            keep = jnp.abs(apart + (n - m) * TILE) >= 2
            ratio = jnp.where(keep, 1.0 - counts_ref[at_m, at_n] / rate, 0.0)
            high, low = high_low(ratio)
            right = b_ref[at_n, :lanes]
            row_sum = jnp.dot(high, right, preferred_element_type=f32)
            row_sum += jnp.dot(low, right, preferred_element_type=f32)
            if n == 0:
                sums_ref[at_m, :] = row_sum
            else:
                sums_ref[at_m, :] += row_sum
            left = at_ref[:, at_m]
            col_sum += jnp.dot(left, high, preferred_element_type=f32)
            col_sum += jnp.dot(left, low, preferred_element_type=f32)
        col_sum = (col_sum[:chunk] + col_sum[chunk:]) * scale
        for k in range(TILE // lanes):
            top = col_sum[:half, k * lanes : (k + 1) * lanes]
            bottom = col_sum[half:, k * lanes : (k + 1) * lanes]
            first = low_lanes(top.shape)
            pair = (
                jnp.where(first, top, swapped(bottom)),
                jnp.where(first, swapped(top), bottom),
            )
            p = n * (TILE // lanes) + k
            own_out[p] = jnp.where(first_core, pair[0], pair[1])
            other_out[p] = jnp.where(first_core, pair[1], pair[0])

    for j in range(rows // chunk):
        sums = sums_ref[pl.ds(j * chunk, chunk), :]
        sums = (sums + swapped(sums)) * scale
        sums = jnp.where(low_lanes((half, lanes)), sums[:half], sums[half:])
        distance = (j % RING - place) & (RING - 1)
        mine = link == j // RING

        @pl.when(mine)
        def _():
            row_own[distance] = sums

        @pl.when(jnp.logical_not(mine))
        def _():
            row_other[distance] = sums


def last_sums(row0_ref, row1_ref, row2_ref, row3_ref, col_ref, row_out, col_out):
    _, lanes = row0_ref.shape

    def unpacked(total):
        return jnp.concatenate([total[:, : lanes // 2], swapped(total)[:, : lanes // 2]], axis=0)

    row_out[...] = unpacked(row0_ref[...] + row1_ref[...] + row2_ref[...] + row3_ref[...])
    total = col_ref[0]
    for k in range(1, col_ref.shape[0]):
        total += col_ref[k]
    col_out[...] = unpacked(total).T


def shards(counts, loadings):
    rows, cols = counts.shape
    chunk, rank = loadings.shape
    nrow = lax.axis_size("row")
    ncol = lax.axis_size("col")
    half = chunk // 2
    pairs = nrow // CORES
    vmem = pl.BlockSpec(memory_space=pltpu.VMEM)
    f32 = jnp.float32

    same_core = [[CORES * p + core for p in range(pairs)] for core in range(CORES)]
    swap = [(r, r ^ 1) for r in range(nrow)]

    def moved_to(row, col):
        _, z, core = place_of(row)
        y = col % RING
        target = (col * nrow + row) // ncol
        target_z = place_of(target)[1]
        return target * ncol + core * RING + (y + 2 - z + target_z) % RING

    to_rows = [
        (row * ncol + col, moved_to(row, col)) for row in range(nrow) for col in range(ncol)
    ]
    across = [(c, c ^ RING) for c in range(ncol)]

    def ring(distance):
        return [
            (link * RING + y, link * RING + (y + distance) % RING)
            for link in range(LINKS)
            for y in range(RING)
        ]

    def around_z(distance):
        return [
            ((x * RING + z) * CORES + core, (x * RING + (z + distance) % RING) * CORES + core)
            for x in range(RING)
            for z in range(RING)
            for core in range(CORES)
        ]

    def around_x(distance):
        return [(r, (r + distance * RING * CORES) % nrow) for r in range(nrow)]

    mine = packed(loadings)
    partner = lax.ppermute(mine, "row", swap)
    both = jnp.stack([mine, partner])
    here = lax.ppermute(both, ("row", "col"), to_rows)
    along = [mine]
    for distance in range(1, RING):
        along.append(lax.ppermute(mine, "row", around_z(distance)))
    along = jnp.stack(along)
    own = [along]
    for distance in range(1, RING):
        own.append(lax.ppermute(along, "row", around_x(distance)))
    around = []
    for distance in range(1, RING):
        around.append(lax.ppermute(here, "col", ring(distance)))
    own = jnp.concatenate(own)
    other = lax.ppermute(own, "row", swap)

    row_own, row_other, own_part, other_part = pl.pallas_call(
        gradients,
        out_shape=(
            jax.ShapeDtypeStruct((RING, half, 2 * rank), f32),
            jax.ShapeDtypeStruct((RING, half, 2 * rank), f32),
            jax.ShapeDtypeStruct((pairs, half, 2 * rank), f32),
            jax.ShapeDtypeStruct((pairs, half, 2 * rank), f32),
        ),
        in_specs=[pl.BlockSpec(memory_space=pltpu.HBM)] + [vmem] * 6,
        out_specs=[vmem] * 4,
        scratch_shapes=[
            pltpu.VMEM((rows, cols), f32),
            pltpu.SemaphoreType.DMA((cols // TILE,)),
            pltpu.VMEM((rows, 4 * rank), jnp.bfloat16),
            pltpu.VMEM((2 * rank, rows), jnp.bfloat16),
            pltpu.VMEM((cols, 4 * rank), jnp.bfloat16),
            pltpu.VMEM((rows, 2 * rank), f32),
        ],
        cost_estimate=pl.CostEstimate(
            flops=2 * rows * cols * rank * 9, bytes_accessed=4 * rows * cols, transcendentals=0
        ),
        compiler_params=pltpu.CompilerParams(vmem_limit_bytes=16 << 20),
        name="gradients",
    )(pltpu.with_memory_space_constraint(counts, pltpu.HBM), here, *around, own, other)

    other_part = lax.ppermute(other_part, "row", swap)
    row_other = lax.ppermute(row_other, "col", across)
    own_part = own_part + other_part
    col_terms = lax.all_to_all(own_part, "row", 0, 0, tiled=True, axis_index_groups=same_core)
    row_own = row_own + row_other
    row_terms = [row_own[0]]
    for distance in range(1, RING):
        row_terms.append(lax.ppermute(row_own[distance], "col", ring(distance)))
    return pl.pallas_call(
        last_sums,
        out_shape=(
            jax.ShapeDtypeStruct((chunk, rank), f32),
            jax.ShapeDtypeStruct((chunk, rank), f32),
        ),
        in_specs=[vmem] * (RING + 1),
        out_specs=[vmem] * 2,
        compiler_params=pltpu.CompilerParams(vmem_limit_bytes=8 << 20),
        name="last_sums",
    )(*row_terms, col_terms)


def solution(mesh):
    return jax.shard_map(
        shards,
        mesh=mesh,
        in_specs=(P("row", "col"), P(("col", "row"), None)),
        out_specs=(P(("row", "col"), None), P(("col", "row"), None)),
        check_vma=False,
    )
```

```python
import jax
import jax.numpy as jnp
from jax import lax
from jax.experimental import pallas as pl
from jax.experimental.pallas import tpu as pltpu
from jax.sharding import PartitionSpec as P


CORES = 2
LINKS = 2
RING = 4
TILE = 512


def packed(chunk):
    half = chunk.shape[0] // 2
    return jnp.concatenate([chunk[:half], chunk[half:]], axis=1)


def low_lanes(shape):
    return lax.broadcasted_iota(jnp.int32, shape, 1) < shape[1] // 2


def swapped(x):
    return pltpu.roll(x, x.shape[1] // 2, 1)


def halves(x):
    low = low_lanes(x.shape)
    turned = swapped(x)
    return jnp.where(low, x, turned), jnp.where(low, turned, x)


def high_low(x):
    high = x.astype(jnp.bfloat16)
    return high, (x - high.astype(jnp.float32)).astype(jnp.bfloat16)


def flip_at(t):
    return t ^ t >> 1


def place_of(row_index):
    return row_index // (RING * CORES), row_index // CORES % RING, row_index % CORES


def gradients(
    counts_hbm, near_ref, far_ref, own_ref, other_ref,
    row_out, own_out, other_out,
    counts_ref, arrived, a_ref, at_ref, b_ref, sums_ref,
):
    rows, cols = counts_ref.shape
    copies = {}
    for n, (start, size) in enumerate(((0, TILE), (TILE, cols - TILE))):
        part = pl.ds(start, size)
        copies[start] = pltpu.make_async_copy(
            counts_hbm.at[:, part], counts_ref.at[:, part], arrived.at[n]
        )
        copies[start].start()
    half, lanes = own_ref.shape[1:]
    chunk = 2 * half
    row_index = lax.axis_index("row")
    col_index = lax.axis_index("col")
    link, place = col_index // RING, col_index % RING
    first_core = row_index % CORES == 0
    scale = 1.0 / (rows * lax.axis_size("row")) ** 0.5
    f32 = jnp.float32

    x, z, core = place_of(row_index)
    home = x % 2 * 2 + z // 2
    for t in range(RING):
        source_z = (z + 2 + home - (place ^ flip_at(t))) & (RING - 1)
        for k in range(CORES):
            ref = (near_ref, far_ref)[t // 2].at[t % 2]
            j = source_z * CORES + (link ^ k)
            for part, twice in enumerate(halves(ref[k])):
                high, low = high_low(twice)
                at = pl.ds(pl.multiple_of(j * chunk + part * half, half), half)
                a_ref[at, :lanes] = high
                a_ref[at, lanes:] = low
    both = jnp.where(
        low_lanes((rows, lanes)), a_ref[:, :lanes].astype(f32), a_ref[:, lanes:].astype(f32)
    )
    at_ref[...] = both.T.astype(jnp.bfloat16)

    for p in range(cols // chunk // CORES):
        source = (x ^ p // RING) * RING + (z ^ flip_at(p % RING))
        for k, ref in enumerate((own_ref, other_ref)):
            j = source * CORES + (core ^ k)
            for part, twice in enumerate(halves(ref[p])):
                high = twice.astype(jnp.bfloat16).astype(f32)
                both = jnp.where(low_lanes(twice.shape), high, twice - high).astype(jnp.bfloat16)
                at = pl.ds(pl.multiple_of(j * chunk + part * half, half), half)
                b_ref[at, :lanes] = both
                b_ref[at, lanes:] = both

    apart = (
        lax.broadcasted_iota(jnp.int32, (TILE, TILE), 1)
        - lax.broadcasted_iota(jnp.int32, (TILE, TILE), 0)
        + (col_index * cols - row_index * rows)
    )
    for n in range(cols // TILE):
        at_n = pl.ds(n * TILE, TILE)
        weights, terms = [], []
        right = b_ref[at_n, :lanes]
        right = jnp.concatenate([right, right], axis=0)
        for m in range(rows // TILE):
            at_m = pl.ds(m * TILE, TILE)
            rate = lax.dot_general(
                a_ref[at_m, :], b_ref[at_n, :], (((1,), (1,)), ((), ())), preferred_element_type=f32
            )
            if m == 0 and n * TILE in copies:
                copies[n * TILE].wait()
            keep = jnp.abs(apart + (n - m) * TILE) >= 2
            ratio = jnp.where(keep, 1.0 - counts_ref[at_m, at_n] / rate, 0.0)
            high, low = high_low(ratio)
            row_sum = jnp.dot(
                jnp.concatenate([high, low], axis=1), right, preferred_element_type=f32
            )
            if n == 0:
                sums_ref[at_m, :] = row_sum
            else:
                sums_ref[at_m, :] += row_sum
            left = at_ref[:, at_m]
            terms += [left, left]
            weights += [high, low]
        col_sum = jnp.dot(
            jnp.concatenate(terms, axis=1), jnp.concatenate(weights, axis=0), preferred_element_type=f32
        )
        col_sum = (col_sum[:chunk] + col_sum[chunk:]) * scale
        for k in range(TILE // lanes):
            top = col_sum[:half, k * lanes : (k + 1) * lanes]
            bottom = col_sum[half:, k * lanes : (k + 1) * lanes]
            first = low_lanes(top.shape)
            pair = (
                jnp.where(first, top, swapped(bottom)),
                jnp.where(first, swapped(top), bottom),
            )
            p = n * (TILE // lanes) + k
            distance = p // RING ^ x, flip_at(p % RING ^ z)
            own_out[distance] = jnp.where(first_core, pair[0], pair[1])
            other_out[distance] = jnp.where(first_core, pair[1], pair[0])

    for j in range(rows // chunk):
        sums = sums_ref[pl.ds(j * chunk, chunk), :]
        sums = (sums + swapped(sums)) * scale
        sums = jnp.where(low_lanes((half, lanes)), sums[:half], sums[half:])
        row_out[flip_at(j % RING ^ place), link ^ j // RING] = sums


def last_sums(row_ref, link_ref, col0_ref, col1_ref, col2_ref, col3_ref, row_out, col_out):
    _, lanes = row_ref.shape

    def unpacked(total):
        return jnp.concatenate([total[:, : lanes // 2], swapped(total)[:, : lanes // 2]], axis=0)

    row_out[...] = unpacked(row_ref[...] + link_ref[...])
    col_out[...] = unpacked(col0_ref[...] + col1_ref[...] + col2_ref[...] + col3_ref[...]).T


def shards(counts, loadings):
    rows, cols = counts.shape
    chunk, rank = loadings.shape
    nrow = lax.axis_size("row")
    ncol = lax.axis_size("col")
    half = chunk // 2
    vmem = pl.BlockSpec(memory_space=pltpu.VMEM)
    f32 = jnp.float32

    swap = [(r, r ^ 1) for r in range(nrow)]

    def moved_to(row, col):
        _, z, core = place_of(row)
        y = col % RING
        target = (col * nrow + row) // ncol
        target_z = place_of(target)[1]
        return target * ncol + core * RING + (y + 2 - z + target_z) % RING

    to_rows = [
        (row * ncol + col, moved_to(row, col)) for row in range(nrow) for col in range(ncol)
    ]
    across = [(c, c ^ RING) for c in range(ncol)]

    def flip_y(flip):
        return [(c, c ^ flip) for c in range(ncol)]

    def flip_z(flip):
        return [(r, r ^ flip * CORES) for r in range(nrow)]

    def flip_x(flip):
        return [(r, r ^ flip * RING * CORES) for r in range(nrow)]

    mine = packed(loadings)
    partner = lax.ppermute(mine, "row", swap)
    both = jnp.stack([lax.optimization_barrier(mine), partner])
    here = lax.ppermute(both, ("row", "col"), to_rows)

    along = jnp.stack([mine, lax.ppermute(mine, "row", flip_z(1))])
    along = jnp.concatenate([along, lax.ppermute(along, "row", flip_z(3))])
    near = jnp.stack([here, lax.ppermute(here, "col", flip_y(1))])
    far = lax.ppermute(near, "col", flip_y(3))
    own = [along]
    for flip in range(1, RING):
        own.append(lax.ppermute(along, "row", flip_x(flip)))
    own = jnp.concatenate(own)
    other = lax.ppermute(own, "row", swap)

    row_part, own_part, other_part = pl.pallas_call(
        gradients,
        out_shape=(
            jax.ShapeDtypeStruct((RING, LINKS, half, 2 * rank), f32),
            jax.ShapeDtypeStruct((RING, RING, half, 2 * rank), f32),
            jax.ShapeDtypeStruct((RING, RING, half, 2 * rank), f32),
        ),
        in_specs=[pl.BlockSpec(memory_space=pltpu.HBM)] + [vmem] * 4,
        out_specs=[vmem] * 3,
        scratch_shapes=[
            pltpu.VMEM((rows, cols), f32),
            pltpu.SemaphoreType.DMA((2,)),
            pltpu.VMEM((rows, 4 * rank), jnp.bfloat16),
            pltpu.VMEM((2 * rank, rows), jnp.bfloat16),
            pltpu.VMEM((cols, 4 * rank), jnp.bfloat16),
            pltpu.VMEM((rows, 2 * rank), f32),
        ],
        cost_estimate=pl.CostEstimate(
            flops=2 * rows * cols * rank * 9, bytes_accessed=4 * rows * cols, transcendentals=0
        ),
        compiler_params=pltpu.CompilerParams(vmem_limit_bytes=16 << 20),
        name="gradients",
    )(pltpu.with_memory_space_constraint(counts, pltpu.HBM), near, far, own, other)

    other_part = lax.ppermute(other_part, "row", swap)
    own_part = own_part + other_part
    row_part = row_part[:2] + lax.ppermute(row_part[2:], "col", flip_y(3))
    terms = [own_part[0]]
    for flip in range(1, RING):
        terms.append(lax.ppermute(own_part[flip], "row", flip_x(flip)))
    col_part = sum(terms)
    row_part = row_part[0] + lax.ppermute(row_part[1], "col", flip_y(1))
    terms = [col_part[0]]
    for t in (3, 2, 1):
        terms.append(lax.ppermute(col_part[t], "row", flip_z(flip_at(t))))
    row_link = lax.ppermute(row_part[1], "col", across)
    return pl.pallas_call(
        last_sums,
        out_shape=(
            jax.ShapeDtypeStruct((chunk, rank), f32),
            jax.ShapeDtypeStruct((chunk, rank), f32),
        ),
        in_specs=[vmem] * (2 + RING),
        out_specs=[vmem] * 2,
        compiler_params=pltpu.CompilerParams(vmem_limit_bytes=8 << 20),
        name="last_sums",
    )(row_part[0], row_link, *terms)


def solution(mesh):
    return jax.shard_map(
        shards,
        mesh=mesh,
        in_specs=(P("row", "col"), P(("col", "row"), None)),
        out_specs=(P(("row", "col"), None), P(("col", "row"), None)),
        check_vma=False,
    )
```
